32 devices in a mesh: gx: 2 (over x), gy: 4 (over y, core), gz: 4 (over z).
Axes of the slice: x: 2, y: 2, z: 4, core: 2. Of those that a mesh axis runs over, the one named last changes fastest.
Arguments:
- fields: float32 [6, 32, 64, 512], P(None, 'gx', 'gy', 'gz'), may hold values from -6 to 6
- permittivity: float32 [32, 64, 512], P('gx', 'gy', 'gz'), may hold values from 1 to 4
- donor_owner: int32 [4096, 1], P(('gx', 'gy', 'gz')), may hold values from 0 to 15; in each aligned block of 128 rows (0 to 127, 128 to 255, ...) at most 16 rows name the same one
- donor_base: int32 [4096, 3], P(('gx', 'gy', 'gz')), may hold values from 0 to 127, as said below
- donor_weights: float32 [4096, 15], P(('gx', 'gy', 'gz')), may hold values from -3 to 3
Outputs:
- new_fields: float32 [6, 32, 64, 512], P(None, 'gx', 'gy', 'gz')
- receptor_values: float32 [6, 4096], P(None, ('gx', 'gy', 'gz'))
The draws below stay inside these ranges and needn't reach their ends.
Inputs may be any that keep to these rules, and one draw needn't show every extreme that they name: `donor_owner`: within the 128 rows of one device no owner index is named by more than 16 rows, and one is named by exactly 16. `donor_base`: column 0 lies in 0 to 15, column 1 in 0 to 15, column 2 in 0 to 127.
All inputs are finite; a program needn't handle non-finite values.
Results may differ from the reference program's by a relative error of at most 0.00002.
Values sent between devices are 32-bit elements; how exact they have to be, the bound alone decides.
A program may use at most 192 MiB of HBM per device.

```python
import math
import jax
import jax.numpy as jnp
import numpy as np
from jax import lax

CX = 16
CY = 16
CZ = 128
R_DEV = 128
CAP = 16
NX = 32
NY = 64
NZ = 512
RECEPT = 4096
N_GY = 4
N_GZ = 4
DEVICES = 32


def draw_donor_base(key, part):
    first = jax.random.randint(jax.random.fold_in(key, 11), (RECEPT, 1), 0, CX, dtype=jnp.int32)
    second = jax.random.randint(jax.random.fold_in(key, 12), (RECEPT, 1), 0, CY, dtype=jnp.int32)
    third = jax.random.randint(jax.random.fold_in(key, 13), (RECEPT, 1), 0, CZ, dtype=jnp.int32)
    return jnp.concatenate([first, second, third], 1)


def steps_of(rng, extent, pieces, low, largest):
    gain, own = 1.0, jax.random.fold_in(rng, 6)
    for position, blocks in pieces:
        heights = jnp.exp(jax.random.uniform(jax.random.fold_in(own, position), (blocks,), jnp.float32, low / len(pieces), largest / len(pieces)))
        gain = gain * jnp.repeat(heights, extent[position] // blocks).reshape([-1 if axis == position else 1 for axis in range(len(extent))])
    return gain


def shared_out(stream_key, own, number, rows, amount, top, most, lean):
    sequence = jax.random.permutation(stream_key, amount)
    packed, common = shares(amount, rows * top, most, lean, True), shares(amount, rows * top, most, lean, False)
    places = jnp.arange(amount)

    def named(tallies, offset_by):
        used = int((tallies > 0).sum())
        fixed = max(1, used // 4)
        passed = fixed + (places - fixed + offset_by * (used - fixed)) % max(1, amount - fixed)
        return jnp.zeros((amount,), jnp.int32).at[sequence[jnp.where(places < fixed, places, passed)]].set(jnp.asarray(tallies, jnp.int32))

    tallies = jnp.where(number % 4 == 0, named(packed, number // 4), named(common, number - number // 4 - 1))
    mixed = jax.random.permutation(jax.random.fold_in(own, 3), amount)
    source_of, sink = mixed[0:amount // 2 * 2:2], mixed[1:amount // 2 * 2:2]
    room = jnp.minimum(tallies[source_of] - 1, most - tallies[sink]) // 2
    room = jnp.where((source_of == sequence[0]) | (sink == sequence[0]) | (tallies[sink] == 0), 0, jnp.maximum(room, 0))
    passed = jax.random.randint(jax.random.fold_in(own, 4), (amount // 2,), 0, 1 << 20) % (room + 1)
    tallies = tallies.at[source_of].add(-passed).at[sink].add(passed)
    labels = jnp.searchsorted(jnp.cumsum(tallies), jnp.arange(rows * top), side="right").astype(jnp.int32)
    grid = labels.reshape(top, rows).T
    grid = grid[jax.random.permutation(jax.random.fold_in(own, 1), rows)]
    offset_by = jax.random.randint(jax.random.fold_in(own, 2), (rows, 1), 0, top)
    return jnp.take_along_axis(grid, (jnp.arange(top)[None, :] + offset_by) % top, axis=1)


def shares(number_of, total, limit, slope, full):
    portions = [(1 << 20) // math.isqrt(standing ** slope) + 1 for standing in range(1, number_of + 1)]
    largest = limit if full else min(limit, max(-(-total // number_of), total * portions[0] // sum(portions)))
    least = 1 if total - largest >= number_of - 1 else 0
    holding, spare = [largest] + [least] * (number_of - 1), total - largest - least * (number_of - 1)
    while spare > 0:
        movable = [i for i in range(1, number_of) if holding[i] < largest] or [i for i in range(1, number_of) if holding[i] < limit]
        whole, budget = sum([portions[i] for i in movable]), spare
        for i in movable:
            addition = min(limit - holding[i], max(1, budget * portions[i] // whole), spare)
            holding[i] = holding[i] + addition
            spare = spare - addition
    return np.array(holding)


def bell_draw(own_key, shape, scale, most, cuts=(), kind=jnp.bfloat16):
    loudness = steps_of(own_key, shape, cuts, -0.22, 0.18) if cuts else 1.0
    values = jax.random.normal(own_key, shape, jnp.float32) * scale * loudness
    return jnp.minimum(jnp.maximum(values, -most), most).astype(kind)


def setup_inputs(seed: int = 0) -> dict:
    streams_of = jax.random.split(jax.random.key(seed), 6)
    fields = bell_draw(streams_of[0], (6, NX, NY, NZ), 1.0, 6.0, ((1, 2), (2, 4), (3, 4)), jnp.float32)
    permittivity = jnp.clip(jnp.exp(math.log(4.0) - 1.3862944 * jax.random.uniform(streams_of[1], (NX, NY, NZ), jnp.float32) ** steps_of(streams_of[1], (NX, NY, NZ), ((0, 2), (1, 4), (2, 4)), -0.2, 0.2)), 1.0, 4.0)
    donor_owner_keys = jax.random.split(jax.random.fold_in(streams_of[2], 1), RECEPT // R_DEV)
    donor_owner_turns = jax.random.permutation(jax.random.fold_in(streams_of[2], 3), RECEPT // R_DEV)
    donor_owner = jax.vmap(lambda own, number: shared_out(jax.random.fold_in(streams_of[2], 2), own, number, R_DEV, N_GY * N_GZ, 1, CAP, 2))(donor_owner_keys, donor_owner_turns).reshape((RECEPT, 1))
    donor_base = draw_donor_base(jax.random.fold_in(streams_of[5], 71), 0)
    donor_weights = bell_draw(streams_of[4], (RECEPT, 15), 0.5, 3.0, ((0, 32),), jnp.float32)
    return {"fields": fields, "permittivity": permittivity, "donor_owner": donor_owner, "donor_base": donor_base, "donor_weights": donor_weights}


step_size = 0.25


def shifted(field, axis_index, offset):
    window = [slice(2, -2), slice(2, -2), slice(2, -2)]
    length = field.shape[axis_index] - 4
    window[axis_index] = slice(2 + offset, 2 + offset + length)
    return field[tuple(window)]


def derivative(field, axis_index):
    outer = shifted(field, axis_index, -2) - shifted(field, axis_index, 2)
    inner = shifted(field, axis_index, 1) - shifted(field, axis_index, -1)
    return (outer + 8.0 * inner) / 12.0


def curl_rate(padded, coefficient):
    rate_ex = (derivative(padded[5], 1) - derivative(padded[4], 2)) / coefficient
    rate_ey = (derivative(padded[3], 2) - derivative(padded[5], 0)) / coefficient
    rate_ez = (derivative(padded[4], 0) - derivative(padded[3], 1)) / coefficient
    rate_hx = derivative(padded[1], 2) - derivative(padded[2], 1)
    rate_hy = derivative(padded[2], 0) - derivative(padded[0], 2)
    rate_hz = derivative(padded[0], 1) - derivative(padded[1], 0)
    return jnp.stack([rate_ex, rate_ey, rate_ez, rate_hx, rate_hy, rate_hz])


def contract(donor_tiles, weights):
    weight_x = weights[0:5]
    weight_y = weights[5:10]
    weight_z = weights[10:15]
    along_z = jnp.sum(donor_tiles * weight_z[None, None, None, :, :], axis=3)
    along_y = jnp.sum(along_z * weight_y[None, None, :, :], axis=2)
    return jnp.sum(along_y * weight_x[None, :, :], axis=1)


def reference(fields, permittivity, donor_owner, donor_base, donor_weights):
    accumulated = fields
    taylor_term = fields
    for power in range(1, 5):
        padded = jnp.pad(taylor_term, ((0, 0), (2, 2), (2, 2), (2, 2)))
        taylor_term = (step_size / power) * curl_rate(padded, permittivity)
        accumulated = accumulated + taylor_term
    new_fields = accumulated
    donor_grid = jnp.pad(new_fields, ((0, 0), (2, 2), (2, 2), (2, 2)))
    group_size = N_GY * N_GZ
    device_id = jnp.arange(RECEPT, dtype=jnp.int32) // R_DEV
    plane_id = device_id // group_size
    owner_id = donor_owner[:, 0].astype(jnp.int32)
    row_x = plane_id * CX + donor_base[:, 0]
    row_y = (owner_id // N_GZ) * CY + donor_base[:, 1]
    row_z = (owner_id % N_GZ) * CZ + donor_base[:, 2]
    corners = jnp.stack([row_x, row_y, row_z], 1).astype(jnp.int32).reshape(DEVICES, R_DEV, 3)
    weights = donor_weights.reshape(DEVICES, R_DEV, 15)

    def one_block(block_item):
        corner_rows, weight_rows = block_item
        donor_tiles = jax.vmap(
            lambda corner: lax.dynamic_slice(donor_grid, (jnp.int32(0), corner[0], corner[1], corner[2]), (6, 5, 5, 5)),
            out_axes=4)(corner_rows)
        return contract(donor_tiles, weight_rows.T)

    values = lax.map(one_block, (corners, weights))
    receptor_values = jnp.transpose(values, (1, 0, 2)).reshape(6, RECEPT)
    return new_fields, receptor_values
```

```python
import functools

import jax
import jax.numpy as jnp
from jax import lax
from jax.experimental import pallas as pl
from jax.experimental.pallas import tpu as pltpu
from jax.sharding import PartitionSpec as P

step_size = 0.25
MESH = pl.DeviceIdType.MESH
Y_COMPS = (0, 2, 3, 5)
Z_COMPS = (0, 1, 3, 4)
F32 = jnp.float32
HI = lax.Precision.HIGHEST


def dot(a, b, dims=((1,), (0,))):
    return lax.dot_general(a, b, (dims, ((), ())), precision=HI, preferred_element_type=F32)


def kernel(
    sizes, fields, eps, owner, data, out, recept,
    T, F, H, inv, ys, yr, zs, zr, yfs, yfr, zfs, zfr,
    req, reqr, ans, ansr, W, wz_in, wz_halo, perm,
    load_sem, send, recv, fsend, frecv, rsend, rrecv, asend, arecv,
):
    nx, ny, nz, cap = sizes
    group = ny * nz
    cx, cy, cz = eps.shape
    x, y, z = lax.axis_index("gx"), lax.axis_index("gy"), lax.axis_index("gz")
    me = y * nz + z
    y0, y1 = 8, 8 + cy

    loads = [
        pltpu.make_async_copy(fields, T.at[0, :, pl.ds(2, cx), pl.ds(8, cy), :], load_sem.at[0]),
        pltpu.make_async_copy(fields, F.at[:, pl.ds(2, cx), pl.ds(8, cy), :], load_sem.at[1]),
        pltpu.make_async_copy(eps, inv, load_sem.at[2]),
    ]
    for copy in loads:
        copy.start()

    def clear(ref):
        ref[...] = jnp.zeros(ref.shape, F32)

    for m in range(4):
        for lo in (0, cx + 2):
            clear(T.at[m, :, pl.ds(lo, 2)])
    for lo in (0, cx + 2):
        clear(F.at[:, pl.ds(lo, 2)])
        clear(H.at[pl.ds(lo, 2)])
    for lo in (0, y1):
        clear(F.at[:, pl.ds(2, cx), pl.ds(lo, 8)])
        clear(H.at[pl.ds(2, cx), pl.ds(lo, 8)])
    for ref in (yr, zr, yfr, zfr):
        clear(ref)

    barrier = pltpu.get_barrier_semaphore()
    others = []
    for d in range(1, group):
        t = lax.rem(me + d, group)
        others.append((x, t // nz, lax.rem(t, nz)))
    for target in others:
        pl.semaphore_signal(barrier, inc=1, device_id=target, device_id_type=MESH)

    has = {"xl": x > 0, "xh": x < nx - 1, "yl": y > 0, "yh": y < ny - 1, "zl": z > 0, "zh": z < nz - 1}
    dev = {
        "xl": (x - 1, y, z), "xh": (x + 1, y, z), "yl": (x, y - 1, z), "yh": (x, y + 1, z),
        "zl": (x, y, z - 1), "zh": (x, y, z + 1),
    }
    for side in ("xl", "xh"):
        @pl.when(has[side])
        def _():
            pl.semaphore_signal(barrier, inc=1, device_id=dev[side], device_id_type=MESH)

    rows = owner.shape[0]
    col = lax.broadcasted_iota(jnp.int32, (rows, 128), 1)
    row = lax.broadcasted_iota(jnp.int32, (rows, 128), 0)
    own = owner[...]
    hits = (own == col).astype(F32)
    earlier = dot((lax.broadcasted_iota(jnp.int32, (rows, rows), 1)
                   < lax.broadcasted_iota(jnp.int32, (rows, rows), 0)).astype(F32), hits)
    slot = jnp.sum(earlier * hits, axis=1, keepdims=True).astype(jnp.int32)
    flat = own * cap + slot
    slots = group * cap
    perm[...] = (flat == lax.broadcasted_iota(jnp.int32, (rows, slots), 1)).astype(F32)
    packed = dot(perm[...], data[...], ((0,), (0,)))
    for o in range(group):
        req[o] = packed[o * cap:(o + 1) * cap]
    reqr[me] = req[me]

    for copy in loads:
        copy.wait()
    inv[...] = 1.0 / (12.0 * inv[...])

    pl.semaphore_wait(barrier, group - 1 + has["xl"].astype(jnp.int32) + has["xh"].astype(jnp.int32))

    def remote(src, dst, s, r, target):
        return pltpu.make_async_remote_copy(
            src_ref=src, dst_ref=dst, send_sem=s, recv_sem=r, device_id=target, device_id_type=MESH)

    def request(d):
        return remote(req.at[(me + d) % group], reqr.at[me], rsend.at[d], rrecv.at[d], others[d - 1])

    def answer(d):
        return remote(ans.at[(me + d) % group], ansr.at[me], asend.at[d], arecv.at[d], others[d - 1])

    lane = lax.broadcasted_iota(jnp.int32, (cy, cz), 1)
    opposite = {"xl": "xh", "xh": "xl", "yl": "yh", "yh": "yl", "zl": "zh", "zh": "zl"}

    def x_copies(m, side):
        lo_src, lo_dst = (2, cx + 2) if side == "xl" else (cx, 0)
        base = 0 if side == "xl" else 2
        return [
            remote(T.at[m, pl.ds(c, 2), pl.ds(lo_src, 2), pl.ds(8, cy)],
                   T.at[m, pl.ds(c, 2), pl.ds(lo_dst, 2), pl.ds(8, cy)],
                   send.at[m, base + i], recv.at[m, base + i], dev[side])
            for i, c in enumerate((1, 4))
        ]

    def y_copies(m, side):
        k = 0 if side == "yl" else 1
        return [remote(ys.at[m, k], yr.at[m, k], send.at[m, 4 + k], recv.at[m, 4 + k], dev[side])]

    def z_copies(m, side):
        k = 0 if side == "zl" else 1
        return [remote(zs.at[m], zr.at[m, k], send.at[m, 6 + k], recv.at[m, 6 + k], dev[side])]

    def start(copies, side):
        @pl.when(has[side])
        def _():
            for copy in copies:
                copy.start()

    def finish_recv(copies, side):
        @pl.when(has[opposite[side]])
        def _():
            for copy in copies:
                copy.wait_recv()

    def finish_send(copies, side):
        @pl.when(has[side])
        def _():
            for copy in copies:
                copy.wait_send()

    def shifts_z(f, edge):
        lo2 = pltpu.roll(jnp.where(lane >= cz - 2, edge, f), 2, 1)
        lo1 = pltpu.roll(jnp.where(lane >= cz - 1, edge, f), 1, 1)
        hi2 = pltpu.roll(jnp.where(lane < 2, edge, f), cz - 2, 1)
        hi1 = pltpu.roll(jnp.where(lane < 1, edge, f), cz - 1, 1)
        return (lo2 - hi2) + 8.0 * (hi1 - lo1)

    per = cz // 16

    def step(m, carry):
        for side in ("xl", "xh"):
            start(x_copies(m, side), side)

        def pack(g, c_):
            strip = jnp.zeros((cy, cz), F32)
            for i in range(per):
                px = 2 + g * per + i
                for q, c in enumerate(Z_COMPS):
                    b = (i * 4 + q) * 4
                    strip = jnp.where(lane // 4 == i * 4 + q,
                                      pltpu.roll(T[m, c, px, y0:y1, :], (b + 2) % cz, 1), strip)
            zs[m, g] = strip
            return c_

        lax.fori_loop(0, cx // per, pack, 0)
        for side in ("zl", "zh"):
            start(z_copies(m, side), side)
        for q, c in enumerate(Y_COMPS):
            ys[m, 0, :, 2 * q:2 * q + 2, :] = T[m, c, 2:2 + cx, y0:y0 + 2, :]
            ys[m, 1, :, 2 * q:2 * q + 2, :] = T[m, c, 2:2 + cx, y1 - 2:y1, :]
        for side in ("yl", "yh"):
            start(y_copies(m, side), side)

        @pl.when(m == 0)
        def _():
            for d in range(1, group):
                request(d).start()

        for side in ("zl", "zh"):
            finish_recv(z_copies(m, side), side)
        for side in ("yl", "yh"):
            finish_recv(y_copies(m, side), side)
        for side in ("xl", "xh"):
            finish_recv(x_copies(m, side), side)
        for q, c in enumerate(Y_COMPS):
            T[m, c, 2:2 + cx, y0 - 2:y0, :] = yr[m, 1, :, 2 * q:2 * q + 2, :]
            T[m, c, 2:2 + cx, y1:y1 + 2, :] = yr[m, 0, :, 2 * q:2 * q + 2, :]
        scale = step_size / (m + 1).astype(F32)

        def planes(g, c_):
            merged = jnp.where(lane % 4 < 2, zr[m, 1, g], zr[m, 0, g])
            for i in range(per):
                px = 2 + g * per + i

                def d_x(c):
                    at = lambda o: T[m, c, px + o, y0:y1, :]
                    return (at(-2) - at(2)) + 8.0 * (at(1) - at(-1))

                def d_y(c):
                    at = lambda o: T[m, c, px, y0 + o:y1 + o, :]
                    return (at(-2) - at(2)) + 8.0 * (at(1) - at(-1))

                def d_z(c):
                    b = (i * 4 + Z_COMPS.index(c)) * 4
                    edge = pltpu.roll(merged, (2 * cz - b - 2) % cz, 1)
                    return shifts_z(T[m, c, px, y0:y1, :], edge)

                se = inv[px - 2] * scale
                sh = scale / 12.0
                rates = (
                    (d_y(5) - d_z(4)) * se,
                    (d_z(3) - d_x(5)) * se,
                    (d_x(4) - d_y(3)) * se,
                    (d_z(1) - d_y(2)) * sh,
                    (d_x(2) - d_z(0)) * sh,
                    (d_y(0) - d_x(1)) * sh,
                )
                for c in range(6):
                    T[m + 1, c, px, y0:y1, :] = rates[c]
                    F[c, px, y0:y1, :] = F[c, px, y0:y1, :] + rates[c]
            return c_

        lax.fori_loop(0, cx // per, planes, 0)
        return carry

    lax.fori_loop(0, 4, step, 0)

    store = pltpu.make_async_copy(F.at[:, pl.ds(2, cx), pl.ds(8, cy), :], out, load_sem.at[3])
    store.start()

    def xf_copies(side):
        lo_src, lo_dst = (2, cx + 2) if side == "xl" else (cx, 0)
        base = 0 if side == "xl" else 1
        return [remote(F.at[:, pl.ds(lo_src, 2), pl.ds(8, cy)], F.at[:, pl.ds(lo_dst, 2), pl.ds(8, cy)],
                       fsend.at[base], frecv.at[base], dev[side])]

    def xh_copies(side):
        lo_src, lo_dst = (2, cx + 2) if side == "xl" else (cx, 0)
        base = 2 if side == "xl" else 3
        return [remote(H.at[pl.ds(lo_src, 2), pl.ds(8, cy)], H.at[pl.ds(lo_dst, 2), pl.ds(8, cy)],
                       fsend.at[base], frecv.at[base], dev[side])]

    def yf_copies(side):
        k = 0 if side == "yl" else 1
        return [remote(yfs.at[k], yfr.at[k], fsend.at[4 + k], frecv.at[4 + k], dev[side])]

    def zf_copies(side):
        k = 0 if side == "zl" else 1
        return [remote(zfs, zfr.at[k], fsend.at[6 + k], frecv.at[6 + k], dev[side])]

    for side in ("xl", "xh"):
        start(xf_copies(side), side)
    wide = cz // 32
    for g in range(cx // wide):
        strip = jnp.zeros((cy, cz), F32)
        for i in range(wide):
            for c in range(6):
                b = i * 32 + c * 4
                strip = jnp.where(lane // 4 == b // 4,
                                  pltpu.roll(F[c, 2 + g * wide + i, y0:y1, :], (b + 2) % cz, 1), strip)
        zfs[g] = strip
    for side in ("zl", "zh"):
        start(zf_copies(side), side)

    for d in range(1, group):
        request(d).wait_recv()
    if cap % 8 == 0:
        served = reqr[...].reshape(slots, 128)
    else:
        served = jnp.concatenate([reqr[o] for o in range(group)], axis=0)
    bx = served[:, 0:1].astype(jnp.int32)
    by = served[:, 1:2].astype(jnp.int32)
    bz = served[:, 2:3].astype(jnp.int32)

    def spread(offset, first):
        total = jnp.zeros(offset.shape, F32)
        for k in range(5):
            total = jnp.where(offset == k, served[:, first + k:first + k + 1], total)
        return total

    yrows = F.shape[2]
    for lo in range(0, W.shape[1], 128):
        li = lo + lax.broadcasted_iota(jnp.int32, (slots, 128), 1)
        W[:, lo:lo + 128] = spread(li // yrows - bx, 3) * spread(li % yrows - 6 - by, 8)
    li = lax.broadcasted_iota(jnp.int32, (slots, cz), 1)
    wz_in[...] = spread(li + 2 - bz, 13)
    tail = li % 4
    wz_halo[...] = jnp.where(li < 24, spread(jnp.where(tail < 2, tail, cz + tail) - bz, 13), 0.0)

    for side in ("zl", "zh"):
        finish_recv(zf_copies(side), side)
    for g in range(cx // wide):
        merged = jnp.where(lane % 4 < 2, zfr[1, g], zfr[0, g])
        for i in range(wide):
            H[2 + g * wide + i, y0:y1, :] = pltpu.roll(merged, (cz - i * 32) % cz, 1) if i else merged
    for side in ("xl", "xh"):
        start(xh_copies(side), side)
    for side in ("xl", "xh"):
        finish_recv(xf_copies(side), side)
        finish_recv(xh_copies(side), side)
    for k, lo in ((0, y0), (1, y1 - 2)):
        for c in range(6):
            yfs[k, :, 2 * c:2 * c + 2, :] = F[c, :, lo:lo + 2, :]
        yfs[k, :, 12:14, :] = H[:, lo:lo + 2, :]
    for side in ("yl", "yh"):
        start(yf_copies(side), side)
    for side in ("yl", "yh"):
        finish_recv(yf_copies(side), side)
    for k, lo in ((1, y0 - 2), (0, y1)):
        for c in range(6):
            F[c, :, lo:lo + 2, :] = yfr[k, :, 2 * c:2 * c + 2, :]
        H[:, lo:lo + 2, :] = yfr[k, :, 12:14, :]

    depth = W.shape[1]
    halo = dot(W[...], H[...].reshape(depth, cz)) * wz_halo[...]
    result = jnp.zeros((slots, cz), F32)
    for c in range(6):
        part = dot(W[...], F[c].reshape(depth, cz)) * wz_in[...]
        part = part + jnp.where(li // 4 == c, halo, 0.0)
        result = jnp.where(li == c, jnp.sum(part, axis=1, keepdims=True), result)
    for o in range(group):
        ans[o] = result[o * cap:(o + 1) * cap]
    for d in range(1, group):
        answer(d).start()
    ansr[me] = ans[me]
    for d in range(1, group):
        answer(d).wait_recv()
    if cap % 8 == 0:
        got = ansr[...].reshape(slots, 128)
    else:
        got = jnp.concatenate([ansr[o] for o in range(group)], axis=0)
    picked = dot(perm[...], got)
    recept[...] = jnp.transpose(picked)[0:8, :]

    store.wait()
    for m in range(4):
        for side in ("xl", "xh"):
            finish_send(x_copies(m, side), side)
        for side in ("yl", "yh"):
            finish_send(y_copies(m, side), side)
        for side in ("zl", "zh"):
            finish_send(z_copies(m, side), side)
    for side in ("xl", "xh"):
        finish_send(xf_copies(side), side)
        finish_send(xh_copies(side), side)
    for side in ("yl", "yh"):
        finish_send(yf_copies(side), side)
    for side in ("zl", "zh"):
        finish_send(zf_copies(side), side)
    for d in range(1, group):
        request(d).wait_send()
        answer(d).wait_send()


def local(sizes, fields, permittivity, donor_owner, donor_base, donor_weights):
    nx, ny, nz = sizes
    cx, cy, cz = permittivity.shape
    rows = donor_owner.shape[0]
    group = ny * nz
    cap = 2 * rows // group
    slots = group * cap
    data = jnp.concatenate([donor_base.astype(F32), donor_weights], axis=1)
    data = jnp.pad(data, ((0, 0), (0, 128 - data.shape[1])))
    vmem = pltpu.VMEM
    dma = pltpu.SemaphoreType.DMA
    yrows = cy + 16
    depth = (cx + 4) * yrows
    depth_pad = depth
    out, recept = pl.pallas_call(
        functools.partial(kernel, (nx, ny, nz, cap)),
        out_shape=(
            jax.ShapeDtypeStruct(fields.shape, F32),
            jax.ShapeDtypeStruct((8, rows), F32),
        ),
        in_specs=[
            pl.BlockSpec(memory_space=pl.ANY),
            pl.BlockSpec(memory_space=pl.ANY),
            pl.BlockSpec(memory_space=vmem),
            pl.BlockSpec(memory_space=vmem),
        ],
        out_specs=(pl.BlockSpec(memory_space=pl.ANY), pl.BlockSpec(memory_space=vmem)),
        scratch_shapes=[
            vmem((5, 6, cx + 4, yrows, cz), F32),
            vmem((6, cx + 4, yrows, cz), F32),
            vmem((cx + 4, yrows, cz), F32),
            vmem((cx, cy, cz), F32),
            vmem((4, 2, cx, 8, cz), F32),
            vmem((4, 2, cx, 8, cz), F32),
            vmem((4, cx * 16 // cz, cy, cz), F32),
            vmem((4, 2, cx * 16 // cz, cy, cz), F32),
            vmem((2, cx + 4, 16, cz), F32),
            vmem((2, cx + 4, 16, cz), F32),
            vmem((cx * 32 // cz, cy, cz), F32),
            vmem((2, cx * 32 // cz, cy, cz), F32),
            vmem((group, cap, 128), F32),
            vmem((group, cap, 128), F32),
            vmem((group, cap, 128), F32),
            vmem((group, cap, 128), F32),
            vmem((slots, depth_pad), F32),
            vmem((slots, cz), F32),
            vmem((slots, cz), F32),
            vmem((rows, slots), F32),
            dma((4,)),
            dma((4, 8)),
            dma((4, 8)),
            dma((8,)),
            dma((8,)),
            dma((group,)),
            dma((group,)),
            dma((group,)),
            dma((group,)),
        ],
        compiler_params=pltpu.CompilerParams(
            collective_id=0, has_side_effects=True, vmem_limit_bytes=40 * 1024 * 1024
        ),
    )(fields, permittivity, donor_owner, data)
    return out, recept[0:6]


def solution(mesh):
    sizes = (mesh.shape["gx"], mesh.shape["gy"], mesh.shape["gz"])
    placed = (
        P(None, "gx", "gy", "gz"),
        P("gx", "gy", "gz"),
        P(("gx", "gy", "gz"), None),
        P(("gx", "gy", "gz"), None),
        P(("gx", "gy", "gz"), None),
    )
    return jax.shard_map(
        functools.partial(local, sizes),
        mesh=mesh,
        in_specs=placed,
        out_specs=(P(None, "gx", "gy", "gz"), P(None, ("gx", "gy", "gz"))),
        check_vma=False,
    )
```

```python
import functools

import jax
import jax.numpy as jnp
from jax import lax
from jax.experimental import pallas as pl
from jax.experimental.pallas import tpu as pltpu
from jax.sharding import PartitionSpec as P

step_size = 0.25
MESH = pl.DeviceIdType.MESH
Y_COMPS = (0, 2, 3, 5)
Z_COMPS = (0, 1, 3, 4)
F32 = jnp.float32
HI = lax.Precision.HIGHEST


def dot(a, b, dims=((1,), (0,))):
    return lax.dot_general(a, b, (dims, ((), ())), precision=HI, preferred_element_type=F32)


def split(a):
    hi = a.astype(jnp.bfloat16)
    return hi, (a - hi.astype(F32)).astype(jnp.bfloat16)


def dot16(a, b):
    return lax.dot_general(a, b, (((1,), (0,)), ((), ())), preferred_element_type=F32)


def kernel(
    sizes, fields, eps, owner, bases, weights, out, recept,
    T, F, H, inv, ys, yr, zs, zr, yfs, yfr, zfs, zfr,
    zfd, DZ, E, data_t, inner, outer, req, reqr, ans, ansr, W, W_lo, wz_in, wz_halo, perm,
    load_sem, send, recv, fsend, frecv, rsend, rrecv, asend, arecv, dsend, drecv,
):
    nx, ny, nz, cap = sizes
    group = ny * nz
    cx, cy, cz = eps.shape
    x, y, z = lax.axis_index("gx"), lax.axis_index("gy"), lax.axis_index("gz")
    me = y * nz + z
    y0, y1 = 8, 8 + cy

    loads = [
        pltpu.make_async_copy(fields, T.at[0, :, pl.ds(2, cx), pl.ds(8, cy), :], load_sem.at[0]),
        pltpu.make_async_copy(fields, F.at[:, pl.ds(2, cx), pl.ds(8, cy), :], load_sem.at[1]),
        pltpu.make_async_copy(eps, inv, load_sem.at[2]),
    ]
    for copy in loads:
        copy.start()

    def clear(ref):
        ref[...] = jnp.zeros(ref.shape, F32)

    for m in range(4):
        for lo in (0, cx + 2):
            clear(T.at[m, :, pl.ds(lo, 2)])
    for lo in (0, cx + 2):
        clear(F.at[:, pl.ds(lo, 2)])
        clear(H.at[pl.ds(lo, 2)])
    for lo in (0, y1):
        clear(F.at[:, pl.ds(2, cx), pl.ds(lo, 8)])
        clear(H.at[pl.ds(2, cx), pl.ds(lo, 8)])
    for ref in (yr, zr, yfr, zfr, zfd):
        clear(ref)

    barrier = pltpu.get_barrier_semaphore()
    others = []
    for d in range(1, group):
        t = lax.rem(me + d, group)
        others.append((x, t // nz, lax.rem(t, nz)))
    for target in others:
        pl.semaphore_signal(barrier, inc=1, device_id=target, device_id_type=MESH)

    has = {"xl": x > 0, "xh": x < nx - 1, "yl": y > 0, "yh": y < ny - 1, "zl": z > 0, "zh": z < nz - 1}
    dev = {
        "xl": (x - 1, y, z), "xh": (x + 1, y, z), "yl": (x, y - 1, z), "yh": (x, y + 1, z),
        "zl": (x, y, z - 1), "zh": (x, y, z + 1),
    }
    for side in ("xl", "xh"):
        @pl.when(has[side])
        def _():
            pl.semaphore_signal(barrier, inc=1, device_id=dev[side], device_id_type=MESH)

    corners = [(sx, sz) for sx in ("xl", "xh") for sz in ("zl", "zh")]

    def corner_dev(sx, sz):
        return (dev[sx][0], y, dev[sz][2])

    expected = group - 1 + has["xl"].astype(jnp.int32) + has["xh"].astype(jnp.int32)
    for sx, sz in corners:
        both = has[sx] & has[sz]
        expected = expected + both.astype(jnp.int32)

        @pl.when(both)
        def _():
            pl.semaphore_signal(barrier, inc=1, device_id=corner_dev(sx, sz), device_id_type=MESH)

    rows = owner.shape[1]
    data_t[...] = jnp.zeros(data_t.shape, F32)
    data_t[0:3] = bases[...].astype(F32)
    data_t[3:18] = weights[...]
    data_t[18:19] = owner[...].astype(F32)
    data = jnp.transpose(data_t[...])
    col = lax.broadcasted_iota(jnp.int32, (rows, 128), 1)
    own = data[:, 18:19].astype(jnp.int32)
    hits = (own == col).astype(F32)
    earlier = dot((lax.broadcasted_iota(jnp.int32, (rows, rows), 1)
                   < lax.broadcasted_iota(jnp.int32, (rows, rows), 0)).astype(F32), hits)
    slot = jnp.sum(earlier * hits, axis=1, keepdims=True).astype(jnp.int32)
    flat = own * cap + slot
    slots = group * cap
    perm[...] = (flat == lax.broadcasted_iota(jnp.int32, (rows, slots), 1)).astype(F32)
    packed = dot(perm[...], data, ((0,), (0,)))
    for o in range(group):
        req[o] = packed[o * cap:(o + 1) * cap]
    reqr[me] = req[me]

    for copy in loads:
        copy.wait()
    inv[...] = 1.0 / (12.0 * inv[...])

    zi = lax.broadcasted_iota(jnp.int32, (cz, cz), 0)
    zo = lax.broadcasted_iota(jnp.int32, (cz, cz), 1)

    def stencil(delta):
        return (jnp.where(delta == -2, 1.0, 0.0) - jnp.where(delta == 2, 1.0, 0.0)
                + jnp.where(delta == 1, 8.0, 0.0) - jnp.where(delta == -1, 8.0, 0.0))

    inner[...] = stencil(zi - zo).astype(jnp.bfloat16)
    outer[...] = (stencil(zi - cz - zo) * jnp.where(zi >= cz // 2, 1.0, 0.0)
                  + stencil(zi + cz - zo) * jnp.where(zi < cz // 2, 1.0, 0.0)).astype(jnp.bfloat16)

    pl.semaphore_wait(barrier, expected)

    def remote(src, dst, s, r, target):
        return pltpu.make_async_remote_copy(
            src_ref=src, dst_ref=dst, send_sem=s, recv_sem=r, device_id=target, device_id_type=MESH)

    def request(d):
        return remote(req.at[(me + d) % group], reqr.at[me], rsend.at[d], rrecv.at[d], others[d - 1])

    def answer(d):
        return remote(ans.at[(me + d) % group], ansr.at[me], asend.at[d], arecv.at[d], others[d - 1])

    lane = lax.broadcasted_iota(jnp.int32, (cy, cz), 1)
    opposite = {"xl": "xh", "xh": "xl", "yl": "yh", "yh": "yl", "zl": "zh", "zh": "zl"}

    def x_copies(m, side):
        lo_src, lo_dst = (2, cx + 2) if side == "xl" else (cx, 0)
        base = 0 if side == "xl" else 2
        return [
            remote(T.at[m, pl.ds(c, 2), pl.ds(lo_src, 2), pl.ds(8, cy)],
                   T.at[m, pl.ds(c, 2), pl.ds(lo_dst, 2), pl.ds(8, cy)],
                   send.at[m, base + i], recv.at[m, base + i], dev[side])
            for i, c in enumerate((1, 4))
        ]

    def y_copies(m, side):
        k = 0 if side == "yl" else 1
        return [remote(ys.at[m, k], yr.at[m, k], send.at[m, 4 + k], recv.at[m, 4 + k], dev[side])]

    def z_copies(m, side):
        k = 0 if side == "zl" else 1
        return [remote(zs.at[m], zr.at[m, k], send.at[m, 6 + k], recv.at[m, 6 + k], dev[side])]

    def start(copies, side):
        @pl.when(has[side])
        def _():
            for copy in copies:
                copy.start()

    def finish_recv(copies, side):
        @pl.when(has[opposite[side]])
        def _():
            for copy in copies:
                copy.wait_recv()

    def finish_send(copies, side):
        @pl.when(has[side])
        def _():
            for copy in copies:
                copy.wait_send()

    per = cz // 16

    def step(m, carry):
        for side in ("xl", "xh"):
            start(x_copies(m, side), side)

        def pack(g, c_):
            strip = jnp.zeros((cy, cz), F32)
            for i in range(per):
                px = 2 + g * per + i
                for q, c in enumerate(Z_COMPS):
                    b = (i * 4 + q) * 4
                    strip = jnp.where(lane // 4 == i * 4 + q,
                                      pltpu.roll(T[m, c, px, y0:y1, :], (b + 2) % cz, 1), strip)
            zs[m, g] = strip
            return c_

        lax.fori_loop(0, cx // per, pack, 0)
        for side in ("zl", "zh"):
            start(z_copies(m, side), side)
        for q, c in enumerate(Y_COMPS):
            ys[m, 0, :, 2 * q:2 * q + 2, :] = T[m, c, 2:2 + cx, y0:y0 + 2, :]
            ys[m, 1, :, 2 * q:2 * q + 2, :] = T[m, c, 2:2 + cx, y1 - 2:y1, :]
        for side in ("yl", "yh"):
            start(y_copies(m, side), side)

        @pl.when(m == 0)
        def _():
            for d in range(1, group):
                request(d).start()

        for q, c in enumerate(Z_COMPS):
            hi, lo = split(T[m, c, 2:2 + cx, y0:y1, :].reshape(cx * cy, cz))
            DZ[q] = (dot16(hi, inner[...]) + dot16(lo, inner[...])).reshape(cx, cy, cz)

        for side in ("zl", "zh"):
            finish_recv(z_copies(m, side), side)
        for side in ("yl", "yh"):
            finish_recv(y_copies(m, side), side)
        for side in ("xl", "xh"):
            finish_recv(x_copies(m, side), side)
        for q, c in enumerate(Y_COMPS):
            T[m, c, 2:2 + cx, y0 - 2:y0, :] = yr[m, 1, :, 2 * q:2 * q + 2, :]
            T[m, c, 2:2 + cx, y1:y1 + 2, :] = yr[m, 0, :, 2 * q:2 * q + 2, :]
        scale = step_size / (m + 1).astype(F32)

        def edges(g, c_):
            merged = jnp.where(lane % 4 < 2, zr[m, 1, g], zr[m, 0, g])
            for i in range(per):
                for q in range(4):
                    E[q, g * per + i] = pltpu.roll(merged, (2 * cz - (i * 4 + q) * 4 - 2) % cz, 1)
            return c_

        lax.fori_loop(0, cx // per, edges, 0)
        for q in range(4):
            hi, lo = split(E[q].reshape(cx * cy, cz))
            DZ[q] = DZ[q] + (dot16(hi, outer[...]) + dot16(lo, outer[...])).reshape(cx, cy, cz)

        def planes(g, c_):
            for i in range(per):
                px = 2 + g * per + i

                def d_x(c):
                    at = lambda o: T[m, c, px + o, y0:y1, :]
                    return (at(-2) - at(2)) + 8.0 * (at(1) - at(-1))

                def d_y(c):
                    at = lambda o: T[m, c, px, y0 + o:y1 + o, :]
                    return (at(-2) - at(2)) + 8.0 * (at(1) - at(-1))

                def d_z(c):
                    return DZ[Z_COMPS.index(c), px - 2]

                se = inv[px - 2] * scale
                sh = scale / 12.0
                rates = (
                    (d_y(5) - d_z(4)) * se,
                    (d_z(3) - d_x(5)) * se,
                    (d_x(4) - d_y(3)) * se,
                    (d_z(1) - d_y(2)) * sh,
                    (d_x(2) - d_z(0)) * sh,
                    (d_y(0) - d_x(1)) * sh,
                )
                for c in range(6):
                    T[m + 1, c, px, y0:y1, :] = rates[c]
                    F[c, px, y0:y1, :] = F[c, px, y0:y1, :] + rates[c]
            return c_

        lax.fori_loop(0, cx // per, planes, 0)
        return carry

    lax.fori_loop(0, 4, step, 0)

    store = pltpu.make_async_copy(F.at[:, pl.ds(2, cx), pl.ds(8, cy), :], out, load_sem.at[3])
    store.start()

    def xf_copies(side):
        lo_src, lo_dst = (2, cx + 2) if side == "xl" else (cx, 0)
        base = 0 if side == "xl" else 1
        return [remote(F.at[:, pl.ds(lo_src, 2), pl.ds(8, cy)], F.at[:, pl.ds(lo_dst, 2), pl.ds(8, cy)],
                       fsend.at[base], frecv.at[base], dev[side])]

    last = zfs.shape[0] - 1

    def corner_copy(sx, sz):
        kx, kz = (0 if sx == "xl" else 1), (0 if sz == "zl" else 1)
        return remote(zfs.at[0 if sx == "xl" else last], zfd.at[kx, kz],
                      dsend.at[kx * 2 + kz], drecv.at[kx * 2 + kz], corner_dev(sx, sz))

    def yf_copies(side):
        k = 0 if side == "yl" else 1
        return [remote(yfs.at[k], yfr.at[k], fsend.at[4 + k], frecv.at[4 + k], dev[side])]

    def zf_copies(side):
        k = 0 if side == "zl" else 1
        return [remote(zfs, zfr.at[k], fsend.at[6 + k], frecv.at[6 + k], dev[side])]

    for side in ("xl", "xh"):
        start(xf_copies(side), side)
    wide = cz // 32
    for g in range(cx // wide):
        strip = jnp.zeros((cy, cz), F32)
        for i in range(wide):
            for c in range(6):
                b = i * 32 + c * 4
                strip = jnp.where(lane // 4 == b // 4,
                                  pltpu.roll(F[c, 2 + g * wide + i, y0:y1, :], (b + 2) % cz, 1), strip)
        zfs[g] = strip
    for side in ("zl", "zh"):
        start(zf_copies(side), side)
    for sx, sz in corners:
        @pl.when(has[sx] & has[sz])
        def _():
            corner_copy(sx, sz).start()

    for d in range(1, group):
        request(d).wait_recv()
    if cap % 8 == 0:
        served = reqr[...].reshape(slots, 128)
    else:
        served = jnp.concatenate([reqr[o] for o in range(group)], axis=0)
    bx = served[:, 0:1].astype(jnp.int32)
    by = served[:, 1:2].astype(jnp.int32)
    bz = served[:, 2:3].astype(jnp.int32)

    def spread(offset, first):
        total = jnp.zeros(offset.shape, F32)
        for k in range(5):
            total = jnp.where(offset == k, served[:, first + k:first + k + 1], total)
        return total

    yrows = F.shape[2]
    for lo in range(0, W.shape[1], 128):
        li = lo + lax.broadcasted_iota(jnp.int32, (slots, 128), 1)
        both_xy = spread(li // yrows - bx, 3) * spread(li % yrows - 6 - by, 8)
        W[:, lo:lo + 128], W_lo[:, lo:lo + 128] = split(both_xy)
    li = lax.broadcasted_iota(jnp.int32, (slots, cz), 1)
    wz_in[...] = spread(li + 2 - bz, 13)
    tail = li % 4
    wz_halo[...] = jnp.where(li < 24, spread(jnp.where(tail < 2, tail, cz + tail) - bz, 13), 0.0)

    for side in ("zl", "zh"):
        finish_recv(zf_copies(side), side)
    for g in range(cx // wide):
        merged = jnp.where(lane % 4 < 2, zfr[1, g], zfr[0, g])
        for i in range(wide):
            H[2 + g * wide + i, y0:y1, :] = pltpu.roll(merged, (cz - i * 32) % cz, 1) if i else merged
    for sx, sz in corners:
        @pl.when(has[opposite[sx]] & has[opposite[sz]])
        def _():
            corner_copy(sx, sz).wait_recv()
    for kx, at, shift in ((1, 0, (wide - 2) * 32), (0, cx + 2, 0)):
        merged = jnp.where(lane % 4 < 2, zfd[kx, 1], zfd[kx, 0])
        for i in range(2):
            move = (cz - shift - i * 32) % cz
            H[at + i, y0:y1, :] = pltpu.roll(merged, move, 1) if move else merged
    for side in ("xl", "xh"):
        finish_recv(xf_copies(side), side)
    for k, lo in ((0, y0), (1, y1 - 2)):
        for c in range(6):
            yfs[k, :, 2 * c:2 * c + 2, :] = F[c, :, lo:lo + 2, :]
        yfs[k, :, 12:14, :] = H[:, lo:lo + 2, :]
    for side in ("yl", "yh"):
        start(yf_copies(side), side)
    for side in ("yl", "yh"):
        finish_recv(yf_copies(side), side)
    for k, lo in ((1, y0 - 2), (0, y1)):
        for c in range(6):
            F[c, :, lo:lo + 2, :] = yfr[k, :, 2 * c:2 * c + 2, :]
        H[:, lo:lo + 2, :] = yfr[k, :, 12:14, :]

    depth = W.shape[1]

    def apply(block):
        hi, lo = split(block)
        return dot16(W[...], hi) + dot16(W[...], lo) + dot16(W_lo[...], hi)

    halo = apply(H[...].reshape(depth, cz)) * wz_halo[...]
    result = jnp.zeros((slots, cz), F32)
    for c in range(0, 6, 2):
        pair = apply(jnp.concatenate([F[c].reshape(depth, cz), F[c + 1].reshape(depth, cz)], axis=1))
        for k in range(2):
            part = pair[:, k * cz:(k + 1) * cz] * wz_in[...] + jnp.where(li // 4 == c + k, halo, 0.0)
            result = jnp.where(li == c + k, jnp.sum(part, axis=1, keepdims=True), result)
    for o in range(group):
        ans[o] = result[o * cap:(o + 1) * cap]
    for d in range(1, group):
        answer(d).start()
    ansr[me] = ans[me]
    for d in range(1, group):
        answer(d).wait_recv()
    if cap % 8 == 0:
        got = ansr[...].reshape(slots, 128)
    else:
        got = jnp.concatenate([ansr[o] for o in range(group)], axis=0)
    picked = dot(perm[...], got)
    recept[...] = jnp.transpose(picked)[0:6, :]

    store.wait()
    for m in range(4):
        for side in ("xl", "xh"):
            finish_send(x_copies(m, side), side)
        for side in ("yl", "yh"):
            finish_send(y_copies(m, side), side)
        for side in ("zl", "zh"):
            finish_send(z_copies(m, side), side)
    for side in ("xl", "xh"):
        finish_send(xf_copies(side), side)
    for side in ("yl", "yh"):
        finish_send(yf_copies(side), side)
    for side in ("zl", "zh"):
        finish_send(zf_copies(side), side)
    for sx, sz in corners:
        @pl.when(has[sx] & has[sz])
        def _():
            corner_copy(sx, sz).wait_send()
    for d in range(1, group):
        request(d).wait_send()
        answer(d).wait_send()


def local(sizes, fields, permittivity, donor_owner, donor_base, donor_weights):
    nx, ny, nz = sizes
    cx, cy, cz = permittivity.shape
    rows = donor_owner.shape[0]
    group = ny * nz
    cap = 2 * rows // group
    slots = group * cap
    vmem = pltpu.VMEM
    dma = pltpu.SemaphoreType.DMA
    yrows = cy + 16
    depth = (cx + 4) * yrows
    out, recept = pl.pallas_call(
        functools.partial(kernel, (nx, ny, nz, cap)),
        out_shape=(
            jax.ShapeDtypeStruct(fields.shape, F32),
            jax.ShapeDtypeStruct((6, rows), F32),
        ),
        in_specs=[
            pl.BlockSpec(memory_space=pl.ANY),
            pl.BlockSpec(memory_space=pl.ANY),
            pl.BlockSpec(memory_space=vmem),
            pl.BlockSpec(memory_space=vmem),
            pl.BlockSpec(memory_space=vmem),
        ],
        out_specs=(pl.BlockSpec(memory_space=pl.ANY), pl.BlockSpec(memory_space=vmem)),
        scratch_shapes=[
            vmem((5, 6, cx + 4, yrows, cz), F32),
            vmem((6, cx + 4, yrows, cz), F32),
            vmem((cx + 4, yrows, cz), F32),
            vmem((cx, cy, cz), F32),
            vmem((4, 2, cx, 8, cz), F32),
            vmem((4, 2, cx, 8, cz), F32),
            vmem((4, cx * 16 // cz, cy, cz), F32),
            vmem((4, 2, cx * 16 // cz, cy, cz), F32),
            vmem((2, cx + 4, 16, cz), F32),
            vmem((2, cx + 4, 16, cz), F32),
            vmem((cx * 32 // cz, cy, cz), F32),
            vmem((2, cx * 32 // cz, cy, cz), F32),
            vmem((2, 2, cy, cz), F32),
            vmem((4, cx, cy, cz), F32),
            vmem((4, cx, cy, cz), F32),
            vmem((128, rows), F32),
            vmem((cz, cz), jnp.bfloat16),
            vmem((cz, cz), jnp.bfloat16),
            vmem((group, cap, 128), F32),
            vmem((group, cap, 128), F32),
            vmem((group, cap, 128), F32),
            vmem((group, cap, 128), F32),
            vmem((slots, depth), jnp.bfloat16),
            vmem((slots, depth), jnp.bfloat16),
            vmem((slots, cz), F32),
            vmem((slots, cz), F32),
            vmem((rows, slots), F32),
            dma((4,)),
            dma((4, 8)),
            dma((4, 8)),
            dma((8,)),
            dma((8,)),
            dma((group,)),
            dma((group,)),
            dma((group,)),
            dma((group,)),
            dma((4,)),
            dma((4,)),
        ],
        compiler_params=pltpu.CompilerParams(
            collective_id=0, has_side_effects=True, vmem_limit_bytes=40 * 1024 * 1024
        ),
    )(fields, permittivity, donor_owner.T, donor_base.T, donor_weights.T)
    return out, recept


def solution(mesh):
    sizes = (mesh.shape["gx"], mesh.shape["gy"], mesh.shape["gz"])
    placed = (
        P(None, "gx", "gy", "gz"),
        P("gx", "gy", "gz"),
        P(("gx", "gy", "gz"), None),
        P(("gx", "gy", "gz"), None),
        P(("gx", "gy", "gz"), None),
    )
    return jax.shard_map(
        functools.partial(local, sizes),
        mesh=mesh,
        in_specs=placed,
        out_specs=(P(None, "gx", "gy", "gz"), P(None, ("gx", "gy", "gz"))),
        check_vma=False,
    )
```
